128 devices in a mesh: tp: 4 (over z), dp: 4 (over y), pp: 8 (over x, core).
Axes of the slice: x: 4, y: 4, z: 4, core: 2. Of those that a mesh axis runs over, the one named last changes fastest.
Arguments:
- master: float32 [50304, 768], P('tp')
- exp_avg: float32 [50304, 768], P('tp')
- exp_avg_sq: float32 [50304, 768], P('tp')
- stage_ids: int32 [8, 24, 384], P('pp', 'dp')
- stage_acts: bfloat16 [8, 24, 384, 768], P('pp', 'dp')
Outputs:
- output 1: float32 [50304, 768], P('tp')
- output 2: float32 [50304, 768], P('tp')
- output 3: float32 [50304, 768], P('tp')
- output 4: bfloat16 [50304, 768], P('tp')
All inputs are finite; a program needn't handle non-finite values.
Results may differ from the reference program's by a relative error of at most 0.001.
Values sent between devices are 32-bit elements.
A program may use at most 1 GiB of HBM per device.

```python
import math
import jax
import jax.numpy as jnp
from jax import lax

VOCAB_SIZE = 50304
MODEL_DIM = 768
SEQ_LEN = 384
BATCH_DEV = 6
DATA_REPL = 4
PIPE_STAGES = 8
OPT_STEP = 10
TOKEN_BLOCK = 128

BATCH_ALL = BATCH_DEV * DATA_REPL
TOKENS_REPL = BATCH_DEV * SEQ_LEN
LOG_SPAN = math.ceil(math.log2(VOCAB_SIZE))
LEARN_RATE = 0.003
BETA_ONE = 0.9
BETA_TWO = 0.95
ADAM_EPS = 1e-8
WEIGHT_DECAY = 0.1
CLIP_NORM = 1.0


def draw_ids(key, perm):
    key_exp, key_rank = jax.random.split(key)
    ids_shape = (PIPE_STAGES, BATCH_ALL, SEQ_LEN)
    exponents = jax.random.randint(key_exp, ids_shape, 0, LOG_SPAN + 1)
    upper_bound = jnp.minimum(jnp.left_shift(jnp.int32(1), exponents), VOCAB_SIZE)
    ranks = jax.random.randint(key_rank, ids_shape, 0, upper_bound)
    tokens = perm[ranks]
    tokens = tokens.at[:, 0, 0].set(0)
    tokens = tokens.at[:, BATCH_ALL - 1, SEQ_LEN - 1].set(VOCAB_SIZE - 1)
    return tokens.astype(jnp.int32)


def setup_inputs(seed: int = 0) -> dict:
    key = jax.random.key(seed)
    k_tab, k_avg, k_sq, k_perm, k_ids, k_act, k_hid = jax.random.split(key, 7)
    table_shape = (VOCAB_SIZE, MODEL_DIM)
    elem_scale = (VOCAB_SIZE * MODEL_DIM) ** -0.5
    master = jax.random.normal(k_tab, table_shape, jnp.float32) * MODEL_DIM ** -0.5
    exp_avg = jax.random.normal(k_avg, table_shape, jnp.float32) * (0.3 * elem_scale)
    exp_avg_sq = jnp.exp(0.5 * jax.random.normal(k_sq, table_shape, jnp.float32)) * (0.09 * elem_scale * elem_scale)
    perm = jax.random.permutation(k_perm, VOCAB_SIZE)
    stage_ids = draw_ids(k_ids, perm)
    grad_scale = 0.08 * math.sqrt(DATA_REPL / TOKENS_REPL)
    stage_acts = jax.random.normal(k_act, (PIPE_STAGES, BATCH_ALL, SEQ_LEN, MODEL_DIM), jnp.float32) * grad_scale
    label_pull = math.log(VOCAB_SIZE) / math.sqrt(MODEL_DIM)
    noise = jax.random.normal(k_hid, (BATCH_ALL, SEQ_LEN, MODEL_DIM), jnp.float32)
    hidden = math.sqrt(1.0 - label_pull * label_pull) * noise + (label_pull * math.sqrt(MODEL_DIM)) * master[stage_ids[PIPE_STAGES - 1]]
    stage_acts = stage_acts.at[PIPE_STAGES - 1].set(hidden)
    return {"master": master, "exp_avg": exp_avg, "exp_avg_sq": exp_avg_sq, "stage_ids": stage_ids, "stage_acts": stage_acts.astype(jnp.bfloat16)}


def head_block(table_bf, hid_block, lab_block):
    logits = jnp.dot(hid_block, table_bf.T, preferred_element_type=jnp.float32)
    prob_mat = jax.nn.softmax(logits, axis=-1)
    is_label = lab_block[:, None] == jnp.arange(VOCAB_SIZE, dtype=jnp.int32)[None, :]
    dlogits = (jnp.where(is_label, prob_mat - 1.0, prob_mat) / TOKENS_REPL).astype(jnp.bfloat16)
    return jnp.dot(dlogits.T, hid_block, preferred_element_type=jnp.float32)


def replica_grad(table_bf, ids_in, dx_in, hidden, labels):
    grad_embed = jax.ops.segment_sum(dx_in.astype(jnp.float32), ids_in, num_segments=VOCAB_SIZE)

    def add_block(acc_grad, block_in):
        return acc_grad + head_block(table_bf, block_in[0], block_in[1]), None

    hid_blocks = hidden.reshape(-1, TOKEN_BLOCK, MODEL_DIM)
    lab_blocks = labels.reshape(-1, TOKEN_BLOCK)
    return lax.scan(add_block, grad_embed, (hid_blocks, lab_blocks))[0]


def reference(master, exp_avg, exp_avg_sq, stage_ids, stage_acts):
    table_bf = master.astype(jnp.bfloat16)
    ids_in = stage_ids[0].reshape(DATA_REPL, TOKENS_REPL)
    labels = stage_ids[PIPE_STAGES - 1].reshape(DATA_REPL, TOKENS_REPL)
    dx_in = stage_acts[0].reshape(DATA_REPL, TOKENS_REPL, MODEL_DIM)
    hidden = stage_acts[PIPE_STAGES - 1].reshape(DATA_REPL, TOKENS_REPL, MODEL_DIM)

    def add_replica(acc_grad, block_in):
        return acc_grad + replica_grad(table_bf, block_in[0], block_in[1], block_in[2], block_in[3]), None

    zero_grad = jnp.zeros((VOCAB_SIZE, MODEL_DIM), jnp.float32)
    grad_sum = lax.scan(add_replica, zero_grad, (ids_in, dx_in, hidden, labels))[0]
    gradient = grad_sum / DATA_REPL
    norm_val = jnp.sqrt(jnp.sum(gradient * gradient))
    gradient = gradient * (CLIP_NORM / jnp.maximum(norm_val, CLIP_NORM))
    new_avg = BETA_ONE * exp_avg + (1.0 - BETA_ONE) * gradient
    new_avg_sq = BETA_TWO * exp_avg_sq + (1.0 - BETA_TWO) * gradient * gradient
    corr_one = 1.0 - BETA_ONE ** OPT_STEP
    corr_two = 1.0 - BETA_TWO ** OPT_STEP
    step_dir = (new_avg / corr_one) / (jnp.sqrt(new_avg_sq / corr_two) + ADAM_EPS)
    new_master = master - LEARN_RATE * (step_dir + WEIGHT_DECAY * master)
    return new_master, new_avg, new_avg_sq, new_master.astype(jnp.bfloat16)
```

```python
import functools

import jax
import jax.numpy as jnp
from jax import lax
from jax.experimental import pallas as pl
from jax.experimental.pallas import tpu as pltpu
from jax.sharding import PartitionSpec as P

LEARN_RATE = 0.003
BETA_ONE = 0.9
BETA_TWO = 0.95
ADAM_EPS = 1e-8
WEIGHT_DECAY = 0.1
CLIP_NORM = 1.0
OPT_STEP = 10

MESH = pl.DeviceIdType.MESH
ANY = pl.BlockSpec(memory_space=pl.ANY)
VMEM = pl.BlockSpec(memory_space=pltpu.VMEM)
NEG_BIG = float("-inf")


def barrier_with(axis_sizes):
    barrier = pltpu.get_barrier_semaphore()
    total = 0
    for axis, size in axis_sizes:
        me = lax.axis_index(axis)
        for k in range(1, size):
            pl.semaphore_signal(barrier, inc=1, device_id={axis: lax.rem(me + k, size)}, device_id_type=MESH)
            total += 1
    pl.semaphore_wait(barrier, total)


def in_block(local, block_rows):
    return jnp.where(local < block_rows, local, -(2**30))


def scatter_kernel(n_pp, n_tp, acts, toks, hid_out, dx_out, lab_out, ids_out, stage_bf, stage_f, tok_vm, load_sem, send_sem, recv_sem):
    me = lax.axis_index("pp")
    quarter = stage_f.shape[0]
    piece = quarter // n_pp
    sources = ((0, 0, dx_out, ids_out), (1, n_pp - 1, hid_out, lab_out))
    start = pl.multiple_of(lax.axis_index("tp") * quarter, quarter)
    load_a = pltpu.make_async_copy(acts.at[pl.ds(start, quarter), :], stage_bf, load_sem.at[0])
    load_t = pltpu.make_async_copy(toks, tok_vm, load_sem.at[1])
    load_a.start()
    load_t.start()
    load_a.wait()
    load_t.wait()
    stage_f[...] = stage_bf[...].astype(jnp.float32)
    barrier_with((("pp", n_pp),))
    for which, src, act_out, tok_out in sources:

        def copies(dest, which=which, act_out=act_out, tok_out=tok_out):
            a = pltpu.make_async_remote_copy(
                src_ref=stage_f.at[pl.ds(dest * piece, piece), :],
                dst_ref=act_out,
                send_sem=send_sem.at[which, 0, dest],
                recv_sem=recv_sem.at[which, 0],
                device_id={"pp": dest},
                device_id_type=MESH,
            )
            t = pltpu.make_async_remote_copy(
                src_ref=tok_vm,
                dst_ref=tok_out,
                send_sem=send_sem.at[which, 1, dest],
                recv_sem=recv_sem.at[which, 1],
                device_id={"pp": dest},
                device_id_type=MESH,
            )
            return a, t

        @pl.when(me == src)
        def _(src=src, which=which, act_out=act_out, tok_out=tok_out, copies=copies):
            for dest in range(n_pp):
                if dest != src:
                    for c in copies(dest):
                        c.start()
            own_a = pltpu.make_async_copy(stage_f.at[pl.ds(src * piece, piece), :], act_out, load_sem.at[0])
            own_t = pltpu.make_async_copy(tok_vm, tok_out, load_sem.at[1])
            own_a.start()
            own_t.start()
            own_a.wait()
            own_t.wait()

    for which, src, act_out, tok_out in sources:

        def waits(dest, which=which, act_out=act_out, tok_out=tok_out):
            a = pltpu.make_async_remote_copy(
                src_ref=stage_f.at[pl.ds(dest * piece, piece), :],
                dst_ref=act_out,
                send_sem=send_sem.at[which, 0, dest],
                recv_sem=recv_sem.at[which, 0],
                device_id={"pp": dest},
                device_id_type=MESH,
            )
            t = pltpu.make_async_remote_copy(
                src_ref=tok_vm,
                dst_ref=tok_out,
                send_sem=send_sem.at[which, 1, dest],
                recv_sem=recv_sem.at[which, 1],
                device_id={"pp": dest},
                device_id_type=MESH,
            )
            return a, t

        @pl.when(me == src)
        def _(src=src, waits=waits):
            for dest in range(n_pp):
                if dest != src:
                    for c in waits(dest):
                        c.wait_send()

        @pl.when(me != src)
        def _(src=src, waits=waits):
            other = (src + 1) % n_pp
            for c in waits(other):
                c.wait_recv()


def scatter_sources(acts, toks, n_pp, n_tp):
    tok_count, dim = acts.shape
    quarter = tok_count // n_tp
    piece = quarter // n_pp
    return pl.pallas_call(
        functools.partial(scatter_kernel, n_pp, n_tp),
        out_shape=(
            jax.ShapeDtypeStruct((piece, dim), jnp.float32),
            jax.ShapeDtypeStruct((piece, dim), jnp.float32),
            jax.ShapeDtypeStruct((1, tok_count), jnp.int32),
            jax.ShapeDtypeStruct((1, tok_count), jnp.int32),
        ),
        in_specs=[ANY, ANY],
        out_specs=(ANY, ANY, ANY, ANY),
        scratch_shapes=[
            pltpu.VMEM((quarter, dim), jnp.bfloat16),
            pltpu.VMEM((quarter, dim), jnp.float32),
            pltpu.VMEM((1, tok_count), jnp.int32),
            pltpu.SemaphoreType.DMA((2,)),
            pltpu.SemaphoreType.DMA((2, 2, n_pp)),
            pltpu.SemaphoreType.DMA((2, 2)),
        ],
        compiler_params=pltpu.CompilerParams(collective_id=1, has_side_effects=True),
        name="scatter_sources",
    )(acts, toks)


def dlogits_kernel(
    lay, n_pp, n_tp, block_rows, master, hid, lab, dlog_out, hid_bf_out, e_f, e_bf, h_f, h_bf, logit, dlog, lse, gath_a, gath_b, e_sem, h_sem, out_sem, send_sem, recv_sem
):
    me = lax.axis_index("pp")
    tpi = lax.axis_index("tp")
    chunks, n_dp, piece = lay
    rows_chunk = n_dp * piece
    tok_count, dim = h_f.shape
    tok_tile = min(256, tok_count)
    n_tile = tok_count // tok_tile
    span = n_dp * n_pp * piece
    tail = block_rows % piece

    def first_row(c, d):
        return c * span + (d * n_pp + me) * piece

    def hid_copy(t):
        at = pl.ds(pl.multiple_of(t * tok_tile, tok_tile), tok_tile)
        return pltpu.make_async_copy(hid.at[at, :], h_f.at[at, :], h_sem.at[t])

    def row_copy(c, d, n):
        slot = c * rows_chunk + d * piece
        start = pl.multiple_of(first_row(c, d), 8)
        return pltpu.make_async_copy(master.at[pl.ds(start, n), :], e_f.at[pl.ds(slot, n), :], e_sem.at[c])

    def on_rows(act):
        for c in range(chunks):
            for d in range(n_dp):
                if c * span + (d * n_pp + n_pp - 1) * piece + piece <= block_rows:
                    act(row_copy(c, d, piece))
                else:

                    @pl.when(first_row(c, d) + piece <= block_rows)
                    def _(c=c, d=d):
                        act(row_copy(c, d, piece))

                    if tail:

                        @pl.when(first_row(c, d) + tail == block_rows)
                        def _(c=c, d=d):
                            act(row_copy(c, d, tail))

    on_rows(lambda c: c.start())
    for t in range(n_tile):
        hid_copy(t).start()
    barrier_with((("pp", n_pp), ("tp", n_tp)))
    on_rows(lambda c: c.wait())

    iota_p = lax.broadcasted_iota(jnp.int32, (piece, tok_tile), 0)
    for c in range(chunks):
        for d in range(n_dp):
            at = pl.ds(c * rows_chunk + d * piece, piece)
            rows = e_f[at, :]
            if c * span + (d * n_pp + n_pp - 1) * piece + piece > block_rows:
                inside = lax.broadcasted_iota(jnp.int32, (piece, dim), 0) + first_row(c, d) < block_rows
                rows = jnp.where(inside, rows, 0.0)
            e_bf[at, :] = rows.astype(jnp.bfloat16)

    def logit_tile(t, _):
        at = pl.ds(pl.multiple_of(t * tok_tile, tok_tile), tok_tile)
        hid_copy(t).wait()
        h_tile = h_f[at, :].astype(jnp.bfloat16)
        h_bf[at, :] = h_tile
        top = jnp.full((8, tok_tile), NEG_BIG, jnp.float32)
        for c in range(chunks):
            rows = pl.ds(c * rows_chunk, rows_chunk)
            val = lax.dot_general(e_bf[rows, :], h_tile, (((1,), (1,)), ((), ())), preferred_element_type=jnp.float32)
            for d in range(n_dp):
                part = val[d * piece : (d + 1) * piece]
                if c * span + (d * n_pp + n_pp - 1) * piece + piece > block_rows:
                    part = jnp.where(iota_p + first_row(c, d) < block_rows, part, NEG_BIG)
                logit[pl.ds(c * rows_chunk + d * piece, piece), at] = part
                top = jnp.maximum(top, jnp.max(part.reshape(piece // 8, 8, tok_tile), axis=0))
        top = jnp.max(top, axis=0, keepdims=True)
        total = jnp.zeros((8, tok_tile), jnp.float32)
        for c in range(chunks):
            val = jnp.exp(logit[pl.ds(c * rows_chunk, rows_chunk), at] - top)
            total = total + jnp.sum(val.reshape(rows_chunk // 8, 8, tok_tile), axis=0)
        lse[:, at] = top + jnp.log(jnp.sum(total, axis=0, keepdims=True))
        return 0

    lax.fori_loop(0, n_tile, logit_tile, 0)
    hid_bf_copy = pltpu.make_async_copy(h_bf, hid_bf_out, out_sem.at[chunks])
    hid_bf_copy.start()

    def exchange(axis, size, gathered, stage):
        idx = lax.axis_index(axis)
        sends = []
        for k in range(1, size):
            copy = pltpu.make_async_remote_copy(
                src_ref=lse,
                dst_ref=gathered.at[k],
                send_sem=send_sem.at[stage, k],
                recv_sem=recv_sem.at[stage, k],
                device_id={axis: lax.rem(idx + k, size)},
                device_id_type=MESH,
            )
            copy.start()
            sends.append(copy)
        own = lse[...]
        for copy in sends:
            copy.wait()
        top = own
        for k in range(1, size):
            top = jnp.maximum(top, gathered[k])
        total = jnp.exp(own - top)
        for k in range(1, size):
            total = total + jnp.exp(gathered[k] - top)
        lse[...] = top + jnp.log(total)

    exchange("pp", n_pp, gath_a, 0)
    exchange("tp", n_tp, gath_b, 1)

    inv_tok = 1.0 / tok_count
    vocab_base = tpi * block_rows

    for c in range(chunks):

        def dlog_tile(t, _, c=c):
            at = pl.ds(pl.multiple_of(t * tok_tile, tok_tile), tok_tile)
            norm = lse[:, at]
            labels = in_block(lab[:, at] - vocab_base, block_rows)
            for d in range(n_dp):
                rows = pl.ds(c * rows_chunk + d * piece, piece)
                prob = jnp.exp(logit[rows, at] - norm)
                hit = iota_p == labels - first_row(c, d)
                dlog[rows, at] = (jnp.where(hit, prob - 1.0, prob) * inv_tok).astype(jnp.bfloat16)
            return 0

        lax.fori_loop(0, n_tile, dlog_tile, 0)
        rows = pl.ds(c * rows_chunk, rows_chunk)
        pltpu.make_async_copy(dlog.at[rows, :], dlog_out.at[rows, :], out_sem.at[c]).start()
    for c in range(chunks):
        rows = pl.ds(c * rows_chunk, rows_chunk)
        pltpu.make_async_copy(dlog.at[rows, :], dlog_out.at[rows, :], out_sem.at[c]).wait()
    hid_bf_copy.wait()


def head_dlogits(master, hid, lab, lay, n_pp, n_tp):
    chunks, n_dp, piece = lay
    rows = chunks * n_dp * piece
    tok_count, dim = hid.shape
    n_tile = tok_count // min(256, tok_count)
    return pl.pallas_call(
        functools.partial(dlogits_kernel, lay, n_pp, n_tp, master.shape[0]),
        out_shape=(jax.ShapeDtypeStruct((rows, tok_count), jnp.bfloat16), jax.ShapeDtypeStruct((tok_count, dim), jnp.bfloat16)),
        in_specs=[ANY, ANY, VMEM],
        out_specs=(ANY, ANY),
        scratch_shapes=[
            pltpu.VMEM((rows, dim), jnp.float32),
            pltpu.VMEM((rows, dim), jnp.bfloat16),
            pltpu.VMEM((tok_count, dim), jnp.float32),
            pltpu.VMEM((tok_count, dim), jnp.bfloat16),
            pltpu.VMEM((rows, tok_count), jnp.float32),
            pltpu.VMEM((rows, tok_count), jnp.bfloat16),
            pltpu.VMEM((1, tok_count), jnp.float32),
            pltpu.VMEM((n_pp, 1, tok_count), jnp.float32),
            pltpu.VMEM((n_tp, 1, tok_count), jnp.float32),
            pltpu.SemaphoreType.DMA((chunks,)),
            pltpu.SemaphoreType.DMA((n_tile,)),
            pltpu.SemaphoreType.DMA((chunks + 1,)),
            pltpu.SemaphoreType.DMA((2, n_pp)),
            pltpu.SemaphoreType.DMA((2, n_pp)),
        ],
        compiler_params=pltpu.CompilerParams(collective_id=2, has_side_effects=True, vmem_limit_bytes=58 * 2**20),
        cost_estimate=pl.CostEstimate(flops=20 * 10**9, bytes_accessed=25 * 10**6, transcendentals=8 * 10**6),
        name="head_dlogits",
    )(master, hid, lab)


def grad_kernel(chunk, lay, n_pp, block_rows, dlog, hid_bf, dx, ids, out):
    chunks, n_dp, piece = lay
    t = pl.program_id(0)
    me = lax.axis_index("pp")
    tok = in_block(ids[...] - lax.axis_index("tp") * block_rows, block_rows)
    tok = tok - (chunk * n_dp * n_pp * piece + me * piece)
    iota_p = lax.broadcasted_iota(jnp.int32, (piece, ids.shape[1]), 0)
    one_hot = jnp.concatenate(
        [jnp.where(iota_p == tok - d * n_pp * piece, 1.0, 0.0).astype(jnp.bfloat16) for d in range(n_dp)], axis=0
    )
    val = jnp.dot(dlog[...], hid_bf[...], preferred_element_type=jnp.float32)
    val = val + jnp.dot(one_hot, dx[...].astype(jnp.bfloat16), preferred_element_type=jnp.float32)

    @pl.when(t == 0)
    def _():
        out[...] = val

    @pl.when(t != 0)
    def _():
        out[...] += val


def chunk_grad(dlog, hid_bf, dx, ids, chunk, lay, n_pp, block_rows):
    chunks, n_dp, piece = lay
    rows = n_dp * piece
    tok_count, dim = hid_bf.shape
    tile = min(256, tok_count)
    return pl.pallas_call(
        functools.partial(grad_kernel, chunk, lay, n_pp, block_rows),
        grid=(tok_count // tile,),
        out_shape=jax.ShapeDtypeStruct((rows, dim), jnp.float32),
        in_specs=[
            pl.BlockSpec((rows, tile), lambda t: (chunk, t)),
            pl.BlockSpec((tile, dim), lambda t: (t, 0)),
            pl.BlockSpec((tile, dim), lambda t: (t, 0)),
            pl.BlockSpec((1, tile), lambda t: (0, t)),
        ],
        out_specs=pl.BlockSpec((rows, dim), lambda t: (0, 0)),
        cost_estimate=pl.CostEstimate(flops=3 * 10**9, bytes_accessed=13 * 10**6, transcendentals=0),
        name=f"grad_{chunk}",
    )(dlog, hid_bf, dx, ids)


def adamw_kernel(n_prev, factor, grad, master, avg, avg_sq, *refs):
    new_master, new_avg, new_sq, new_bf = refs[n_prev:]
    g = grad[...] * factor[0, 0]
    m = BETA_ONE * avg[...] + (1.0 - BETA_ONE) * g
    v = BETA_TWO * avg_sq[...] + (1.0 - BETA_TWO) * g * g
    step_dir = (m * (1.0 / (1.0 - BETA_ONE**OPT_STEP))) / (jnp.sqrt(v * (1.0 / (1.0 - BETA_TWO**OPT_STEP))) + ADAM_EPS)
    w = master[...]
    w = w - LEARN_RATE * (step_dir + WEIGHT_DECAY * w)
    new_master[...] = w
    new_avg[...] = m
    new_sq[...] = v
    new_bf[...] = w.astype(jnp.bfloat16)


def tile_of(rows, most):
    return max(t for t in range(8, most + 1, 8) if rows % t == 0)


def chunk_update(factor, grad, master, avg, avg_sq, prev, row0):
    dim = grad.shape[1]
    rows = min(grad.shape[0], master.shape[0] - row0)
    tile = tile_of(rows, 640)
    table = pl.BlockSpec((pl.Element(tile), pl.Element(dim)), lambda i: (pl.multiple_of(row0 + i * tile, 8), 0))
    grad_spec = pl.BlockSpec((pl.Element(tile), pl.Element(dim)), lambda i: (pl.multiple_of(i * tile, 8), 0))
    n_prev = len(prev)
    return pl.pallas_call(
        functools.partial(adamw_kernel, n_prev),
        grid=(rows // tile,),
        out_shape=(
            jax.ShapeDtypeStruct(master.shape, jnp.float32),
            jax.ShapeDtypeStruct(master.shape, jnp.float32),
            jax.ShapeDtypeStruct(master.shape, jnp.float32),
            jax.ShapeDtypeStruct(master.shape, jnp.bfloat16),
        ),
        in_specs=[pl.BlockSpec(memory_space=pltpu.SMEM), grad_spec, table, table, table] + [ANY] * n_prev,
        out_specs=(table, table, table, table),
        input_output_aliases={5 + i: i for i in range(n_prev)},
        cost_estimate=pl.CostEstimate(flops=10**10, bytes_accessed=rows * dim * 30, transcendentals=rows * dim),
        name=f"adamw_{row0}",
    )(factor, grad, master, avg, avg_sq, *prev)


def layout_of(block_rows, n_dp, n_pp):
    chunks = 5
    unit = chunks * n_dp * n_pp
    piece = -(-block_rows // unit)
    return chunks, n_dp, -(-piece // 16) * 16


def solution(mesh):
    n_tp, n_dp, n_pp = mesh.shape["tp"], mesh.shape["dp"], mesh.shape["pp"]
    table_spec = P("tp", None)

    def device_step(master, exp_avg, exp_avg_sq, stage_ids, stage_acts):
        block_rows, dim = master.shape
        lay = layout_of(block_rows, n_dp, n_pp)
        chunks, _, piece = lay
        tok_count = stage_ids.shape[1] * stage_ids.shape[2]
        toks = stage_ids.reshape(1, tok_count)
        acts = stage_acts.reshape(tok_count, dim)
        hid_piece, dx_piece, lab, ids = scatter_sources(acts, toks, n_pp, n_tp)
        hid = lax.all_gather(hid_piece, ("tp", "pp"), axis=0, tiled=True)
        dx = lax.all_gather(dx_piece, ("tp", "pp"), axis=0, tiled=True)
        dlog, hid_bf = head_dlogits(master, hid, lab, lay, n_pp, n_tp)
        shards = []
        for c in range(chunks):
            part = chunk_grad(dlog, hid_bf, dx, ids, c, lay, n_pp, block_rows)
            shards.append(lax.psum_scatter(part, "dp", scatter_dimension=0, tiled=True))
        sq_sum = sum(jnp.sum(s * s) for s in shards)
        sq_total = lax.psum(sq_sum, ("tp", "dp", "pp")) / (n_dp * n_dp)
        factor = (CLIP_NORM / jnp.maximum(jnp.sqrt(sq_total), CLIP_NORM)) / n_dp
        factor = factor.reshape(1, 1)
        outs = ()
        span = n_dp * n_pp * piece
        for c in range(chunks):
            grad = lax.all_gather(shards[c], ("dp", "pp"), axis=0, tiled=True)
            outs = tuple(chunk_update(factor, grad, master, exp_avg, exp_avg_sq, outs, c * span))
        return outs

    specs = (table_spec, table_spec, table_spec, P("pp", "dp", None), P("pp", "dp", None, None))
    return jax.shard_map(device_step, mesh=mesh, in_specs=specs, out_specs=(table_spec,) * 4, check_vma=False)
```

```python
import functools

import jax
import jax.numpy as jnp
from jax import lax
from jax.experimental import pallas as pl
from jax.experimental.pallas import tpu as pltpu
from jax.sharding import PartitionSpec as P


LEARN_RATE = 0.003
BETA_ONE = 0.9
BETA_TWO = 0.95
ADAM_EPS = 1e-8
WEIGHT_DECAY = 0.1
CLIP_NORM = 1.0
OPT_STEP = 10


MESH = pl.DeviceIdType.MESH
ANY = pl.BlockSpec(memory_space=pl.ANY)
VMEM = pl.BlockSpec(memory_space=pltpu.VMEM)
NEG_BIG = float("-inf")


def in_block(local, block_rows):
    return jnp.where(local < block_rows, local, -(2**30))


def remote(src, dst, send_sem, recv_sem, device):
    return pltpu.make_async_remote_copy(
        src_ref=src, dst_ref=dst, send_sem=send_sem, recv_sem=recv_sem, device_id=device, device_id_type=MESH
    )


LANE = 128
PIECE_TOK = 64


def front_kernel(
    cfg, master, acts, toks, *refs
):
    n_tp, n_dp, n_pp, chunks, bases, piece, block_rows = cfg
    group_outs, factor_out = refs[:4], refs[4]
    (h_f, x_f, h_bf, x_bf, part, e_bf, logit, dlog, lse, lse_a, lse_b, rs_a, rs_b, lab, ids, sq, sq_all, fac) = refs[5:23]
    (e_sem, load_sem, tok_send, tok_recv, st_recv, d2d_send, x_send, z_send, lse_send, lse_recv, rs_send, rs_recv, sq_send, sq_recv, out_sem) = refs[23:38]
    (f_send, f_recv, p_send, p_recv, ready) = refs[38:]
    me = lax.axis_index("pp")
    tpi = lax.axis_index("tp")
    dpi = lax.axis_index("dp")
    n_x = n_pp // 2
    x, core = me // 2, lax.rem(me, 2)
    n_chunk = len(chunks)
    rows_chunk = n_dp * piece
    tok_count, dim = h_f.shape
    half_tok = tok_count // 2
    tiles_a = (half_tok // LANE + 1) // 2
    tiles_b = half_tok // LANE - tiles_a
    per_tile = LANE // PIECE_TOK
    counts = (tiles_a * per_tile, tiles_b * per_tile) * 2
    tok_a = tiles_a * LANE

    def row_at(c, d, x_at, core_at):
        color, s, count = chunks[c]
        owner = d * n_pp + x_at * 2 + core_at if color == 0 else x_at * (2 * n_dp) + d * 2 + core_at
        return bases[color] + (owner * count + s) * piece

    def first_row(c, d):
        return row_at(c, d, x, core)

    def whole(c, d):
        return row_at(c, d, n_x - 1, 1) + piece <= block_rows

    tail = block_rows % piece

    def row_copy(c, d, n):
        slot = c * rows_chunk + d * piece
        start = pl.multiple_of(first_row(c, d), 8)
        return pltpu.make_async_copy(master.at[pl.ds(start, n), :], part.at[pl.ds(slot, n), :], e_sem.at[c])

    def on_rows(act):
        for c in range(n_chunk):
            for d in range(n_dp):
                if whole(c, d):
                    act(row_copy(c, d, piece))
                else:

                    @pl.when(first_row(c, d) + piece <= block_rows)
                    def _(c=c, d=d):
                        act(row_copy(c, d, piece))

                    if tail:

                        @pl.when(first_row(c, d) + tail == block_rows)
                        def _(c=c, d=d):
                            act(row_copy(c, d, tail))

    src_h = me == n_pp - 1
    src_x = me == 0

    def source_loads(buf, tok):
        return (pltpu.make_async_copy(acts, buf, load_sem.at[0]), pltpu.make_async_copy(toks, tok, load_sem.at[1]))

    for is_src, buf, tok in ((src_h, h_bf, lab), (src_x, x_bf, ids)):

        @pl.when(is_src)
        def _(buf=buf, tok=tok):
            for c in source_loads(buf, tok):
                c.start()

    on_rows(lambda c: c.start())
    barrier = pltpu.get_barrier_semaphore()
    for axis, idx, size in (("pp", me, n_pp), ("tp", tpi, n_tp), ("dp", dpi, n_dp)):
        for k in range(1, size):
            pl.semaphore_signal(barrier, inc=1, device_id={axis: lax.rem(idx + k, size)}, device_id_type=MESH)

    for is_src, buf, tok, wide in ((src_h, h_bf, lab, h_f), (src_x, x_bf, ids, x_f)):

        @pl.when(is_src)
        def _(buf=buf, tok=tok, wide=wide):
            for c in source_loads(buf, tok):
                c.wait()

            def widen(t, _):
                at = pl.ds(pl.multiple_of(t * LANE, LANE), LANE)
                wide[at, :] = buf[at, :].astype(jnp.float32)
                return 0

            lax.fori_loop(0, tok_count // LANE, widen, 0)

    pl.semaphore_wait(barrier, n_pp + n_tp + n_dp - 3)

    def tok_copy(which, ref, k):
        return remote(ref, ref, tok_send.at[which, k], tok_recv.at[which], {"pp": lax.rem(me + k, n_pp)})

    for which, is_src, tok in ((0, src_h, lab), (1, src_x, ids)):

        @pl.when(is_src)
        def _(which=which, tok=tok):
            for k in range(1, n_pp):
                tok_copy(which, tok, k).start()

    half = lax.rem(tpi, 2)
    partner = {"pp": x * 2 + 1 - core}
    right = {"pp": lax.rem(x + 1, n_x) * 2 + core}
    left = {"pp": lax.rem(x + n_x - 1, n_x) * 2 + core}
    z_up = {"tp": lax.rem(tpi + 1, n_tp)}
    z_down = {"tp": lax.rem(tpi + n_tp - 1, n_tp)}
    hop = 2 * per_tile // 2
    lag = (hop * (n_x - 2) + hop) // per_tile + 1

    def stream(s, buf):
        handler = core == 1 - s
        u = lax.rem(x - (n_x - 1, 0)[s] + n_x, n_x)
        base = [half * half_tok, half * half_tok + tok_a, (1 - half) * half_tok, (1 - half) * half_tok + tok_a]
        ahead = jnp.maximum(u - 1, 0) * hop
        behind = jnp.where(u == 0, 0, (n_x - 1 - u) * hop)
        second = jnp.where(u == 0, 0, hop)
        offs = (ahead, behind, ahead + second, behind + second)

        def rows(kind, p, n):
            return buf.at[pl.ds(pl.multiple_of(base[kind] + p * PIECE_TOK, PIECE_TOK), n), :]

        def copy(kind, p, to, sem, device, n=PIECE_TOK):
            at = rows(kind, p, n)
            return remote(at, at, sem, st_recv.at[s, to, p], device)

        def outs(kind):
            found = [(handler, kind, d2d_send.at[s, kind], partner)]
            if kind == 0:
                found.append((handler & (u <= n_x - 2), 0, x_send.at[s, 0], right))
                found.append((handler & (u > 0), 2, z_send.at[s, 0], z_up))
            if kind == 1:
                found.append((handler & ((u == 0) | (u >= 2)), 1, x_send.at[s, 1], left))
                found.append((handler & (u > 0), 3, z_send.at[s, 1], z_down))
            return found

        def slot(t):
            for kind in range(4):
                p = t - offs[kind]

                @pl.when((p >= 0) & (p < counts[kind]))
                def _(kind=kind, p=p):
                    @pl.when(jnp.logical_not(handler & (u == 0)))
                    def _():
                        copy(kind, p, kind, d2d_send.at[s, kind], partner).wait_recv()

                    for cond, to, sem, device in reversed(outs(kind)):

                        @pl.when(cond)
                        def _(to=to, sem=sem, device=device):
                            copy(kind, p, to, sem, device).start()

        def drain():
            for kind in range(4):
                for cond, to, sem, device in outs(kind):

                    @pl.when(cond)
                    def _(kind=kind, to=to, sem=sem, device=device):
                        copy(kind, 0, to, sem, device, counts[kind] * PIECE_TOK).wait_send()

        return slot, drain

    h_slot, h_drain = stream(0, h_f)
    x_slot, x_drain = stream(1, x_f)
    n_it = lag + tiles_b
    x_first = tiles_a

    def x_it(it):
        for k in range(per_tile):
            x_slot(it * per_tile + k)

    def prepare_rows():
        on_rows(lambda c: c.wait())
        for c in range(n_chunk):
            for d in range(n_dp):
                at = pl.ds(c * rows_chunk + d * piece, piece)
                rows = part[at, :]
                if not whole(c, d):
                    inside = lax.broadcasted_iota(jnp.int32, (piece, dim), 0) + first_row(c, d) < block_rows
                    rows = jnp.where(inside, rows, 0.0)
                e_bf[at, :] = rows.astype(jnp.bfloat16)

    wide_tile = 2 * LANE

    def logit_pair(t_one, t_two):
        ats = [pl.ds(pl.multiple_of(t, LANE), LANE) for t in (t_one, t_two)]
        h_tile = jnp.concatenate([h_f[at, :].astype(jnp.bfloat16) for at in ats], axis=0)
        for i, at in enumerate(ats):
            h_bf[at, :] = h_tile[i * LANE : (i + 1) * LANE]
        top = jnp.full((8, wide_tile), NEG_BIG, jnp.float32)
        iota_p = lax.broadcasted_iota(jnp.int32, (piece, wide_tile), 0)
        for c in range(n_chunk):
            rows = pl.ds(c * rows_chunk, rows_chunk)
            val = lax.dot_general(e_bf[rows, :], h_tile, (((1,), (1,)), ((), ())), preferred_element_type=jnp.float32)
            for d in range(n_dp):
                sub = val[d * piece : (d + 1) * piece]
                if not whole(c, d):
                    sub = jnp.where(iota_p + first_row(c, d) < block_rows, sub, NEG_BIG)
                for i, at in enumerate(ats):
                    logit[pl.ds(c * rows_chunk + d * piece, piece), at] = sub[:, i * LANE : (i + 1) * LANE]
                top = jnp.maximum(top, jnp.max(sub.reshape(piece // 8, 8, wide_tile), axis=0))
        top = jnp.max(top, axis=0, keepdims=True)
        for i, at in enumerate(ats):
            peak = top[:, i * LANE : (i + 1) * LANE]
            total = jnp.zeros((8, LANE), jnp.float32)
            for c in range(n_chunk):
                val = jnp.exp(logit[pl.ds(c * rows_chunk, rows_chunk), at] - peak)
                total = total + jnp.sum(val.reshape(rows_chunk // 8, 8, LANE), axis=0)
            lse[:, at] = peak + jnp.log(jnp.sum(total, axis=0, keepdims=True))

    def h_only(it, _):
        for k in range(per_tile):
            h_slot(it * per_tile + k)
        return 0

    def h_and_logits(it, _):
        j = it - lag
        for k in range(per_tile):
            h_slot(it * per_tile + k)
            x_slot((it - x_first) * per_tile + k)
            if k < 2:
                logit_pair(k * half_tok + j * LANE, k * half_tok + tok_a + j * LANE)
        return 0

    prepare_rows()
    lax.fori_loop(0, lag, h_only, 0)
    lax.fori_loop(lag, n_it, h_and_logits, 0)
    logit_pair((tiles_a - 1) * LANE, half_tok + (tiles_a - 1) * LANE)
    x_done = n_it - x_first

    def lse_copy(axis, idx, size, gathered, stage, k):
        return remote(lse, gathered.at[k], lse_send.at[stage, k], lse_recv.at[stage, k], {axis: lax.rem(idx + k, size)})

    def lse_finish(copies, gathered, size):
        own = lse[...]
        for copy in copies:
            copy.wait()
        top = own
        for k in range(1, size):
            top = jnp.maximum(top, gathered[k])
        total = jnp.exp(own - top)
        for k in range(1, size):
            total = total + jnp.exp(gathered[k] - top)
        lse[...] = top + jnp.log(total)

    for stage, (axis, idx, size, gathered) in enumerate((("pp", me, n_pp, lse_a), ("tp", tpi, n_tp, lse_b))):
        copies = [lse_copy(axis, idx, size, gathered, stage, k) for k in range(1, size)]
        for copy in copies:
            copy.start()
        x_it(x_done + stage)
        lse_finish(copies, gathered, size)
    x_done += 2

    @pl.when(jnp.logical_not(src_h))
    def _():
        tok_copy(0, lab, 1).wait_recv()

    inv_tok = 1.0 / tok_count
    n_wide = tok_count // wide_tile
    iota_w = lax.broadcasted_iota(jnp.int32, (piece, wide_tile), 0)
    vocab_base = tpi * block_rows

    def dlog_chunk(c):
        def tile(t, _):
            at = pl.ds(pl.multiple_of(t * wide_tile, wide_tile), wide_tile)
            norm = lse[:, at]
            labels = in_block(lab[:, at] - vocab_base, block_rows)
            for d in range(n_dp):
                prob = jnp.exp(logit[pl.ds(c * rows_chunk + d * piece, piece), at] - norm)
                hit = iota_w == labels - first_row(c, d)
                dlog[pl.ds(d * piece, piece), at] = (jnp.where(hit, prob - 1.0, prob) * inv_tok).astype(jnp.bfloat16)
            return 0

        lax.fori_loop(0, n_wide, tile, 0)

    def times(tokens, add):
        def go(c):
            rows = pl.ds(c * rows_chunk, rows_chunk)
            val = jnp.dot(dlog[...], tokens[...], preferred_element_type=jnp.float32)
            part[rows, :] = part[rows, :] + val if add else val

        return go

    head = times(h_bf, False)
    look = times(x_bf, True)
    x_its = tiles_a + lag - 1
    for c in range(n_chunk):
        if x_done < x_its:
            x_it(x_done)
            x_done += 1
        dlog_chunk(c)
        head(c)
    while x_done < x_its:
        x_it(x_done)
        x_done += 1

    @pl.when(jnp.logical_not(src_x))
    def _():
        tok_copy(1, ids, 1).wait_recv()

    def narrow(t, _):
        at = pl.ds(pl.multiple_of(t * LANE, LANE), LANE)
        x_bf[at, :] = x_f[at, :].astype(jnp.bfloat16)
        return 0

    lax.fori_loop(0, tok_count // LANE, narrow, 0)

    def one_hot_chunk(c):
        def tile(t, _):
            at = pl.ds(pl.multiple_of(t * wide_tile, wide_tile), wide_tile)
            rows = in_block(ids[:, at] - vocab_base, block_rows)
            for d in range(n_dp):
                hit = iota_w == rows - first_row(c, d)
                dlog[pl.ds(d * piece, piece), at] = jnp.where(hit, 1.0, 0.0).astype(jnp.bfloat16)
            return 0

        lax.fori_loop(0, n_wide, tile, 0)

    up, down, far = lax.rem(dpi + 1, 4), lax.rem(dpi + 3, 4), lax.rem(dpi + 2, 4)
    hd = dim // 2

    def rows_of(c, d):
        return pl.ds(pl.multiple_of(c * rows_chunk + d * piece, 16), piece)

    def rs_one(c):
        return (
            remote(part.at[rows_of(c, far), pl.ds(0, hd)], rs_a.at[c, 0], rs_send.at[0, c, 0], rs_recv.at[0, c, 0], {"dp": up}),
            remote(part.at[rows_of(c, far), pl.ds(hd, hd)], rs_a.at[c, 1], rs_send.at[0, c, 1], rs_recv.at[0, c, 1], {"dp": down}),
        )

    def rs_two(c):
        return (
            remote(part.at[rows_of(c, up), :], rs_b.at[c, 0], rs_send.at[1, c, 0], rs_recv.at[1, c, 0], {"dp": up}),
            remote(part.at[rows_of(c, down), :], rs_b.at[c, 1], rs_send.at[1, c, 1], rs_recv.at[1, c, 1], {"dp": down}),
        )

    def merge(c):
        for copy in rs_one(c):
            copy.wait_recv()
        part[rows_of(c, up), pl.ds(0, hd)] += rs_a[c, 0]
        part[rows_of(c, down), pl.ds(hd, hd)] += rs_a[c, 1]
        for copy in rs_two(c):
            copy.start()

    rings = (
        ("pp", h_f, x, n_x, lambda q: q * 2 + core),
        ("dp", x_f, dpi, n_dp, lambda q: q),
    )

    def block(c, q, core_at, first=0, n=piece):
        color, s, count = chunks[c]
        return rings[color][1].at[pl.ds(pl.multiple_of(((q * 2 + core_at) * count + s) * piece + first, 8), n), :]

    def ring_copy(c, q, way, sem, first=0, n=piece):
        axis, _, idx, size, device = rings[chunks[c][0]]
        to = device(lax.rem(idx + (1 if way == 0 else size - 1), size))
        at = block(c, q, core, first, n)
        return remote(at, at, f_send.at[c, sem], f_recv.at[c, sem], {axis: to})

    def share(c, k):
        _, _, idx, size, _ = rings[chunks[c][0]]
        at = block(c, lax.rem(idx + k, size), core)
        return remote(at, at, p_send.at[c, k], p_recv.at[c, k], partner)

    cut = piece // 2

    def forwards(c):
        _, _, idx, size, _ = rings[chunks[c][0]]
        return (
            ring_copy(c, lax.rem(idx + size - 1, size), 0, 2, 0, cut),
            ring_copy(c, lax.rem(idx + 1, size), 1, 3, cut, piece - cut),
        )

    def owns(c):
        idx = rings[chunks[c][0]][2]
        return ring_copy(c, idx, 0, 0), ring_copy(c, idx, 1, 1)

    def gather_one(c):
        if c == 0:
            pl.semaphore_wait(ready, 5)
        for copy in owns(c):
            copy.start()
        share(c, 0).start()

    def gather_two(c):
        for own, forward, k in zip(owns(c), forwards(c), (3, 1), strict=True):
            own.wait_recv()
            forward.start()
            share(c, k).start()

    def gather_three(c):
        for copy in forwards(c):
            copy.wait_recv()
        share(c, 2).start()

    def gather_four(c):
        for k in range(4):
            share(c, k).wait()
        for copy in owns(c) + forwards(c):
            copy.wait_send()

    def final(c):
        for copy in rs_two(c):
            copy.wait_recv()
        val = part[rows_of(c, dpi), :] + rs_b[c, 0] + rs_b[c, 1]
        color, s, count = chunks[c]
        own = (rings[color][2] * 2 + core) * count + s
        rings[color][1][pl.ds(pl.multiple_of(own * piece, 8), piece), :] = val
        squares = val * val
        squares = jnp.sum(squares.reshape(piece // 8, 8, dim), axis=0)
        tile = squares[:, :LANE]
        for i in range(1, dim // LANE):
            tile = tile + squares[:, i * LANE : (i + 1) * LANE]
        sq[...] = tile if c == 0 else sq[...] + tile

    h_drain()
    x_drain()
    for device in (right, left, partner, {"dp": up}, {"dp": down}):
        pl.semaphore_signal(ready, inc=1, device_id=device, device_id_type=MESH)

    for c in range(n_chunk + 4):
        if c < n_chunk:
            one_hot_chunk(c)
            look(c)
            for copy in rs_one(c):
                copy.start()
        if 0 <= c - 2 < n_chunk:
            merge(c - 2)
        if 0 <= c - 4 < n_chunk:
            final(c - 4)
            gather_one(c - 4)
        if 0 <= c - 5 < n_chunk:
            gather_two(c - 5)
        if 0 <= c - 6 < n_chunk:
            gather_three(c - 6)

    at = 0
    for axis, idx, size in (("pp", me, n_pp), ("tp", tpi, n_tp), ("dp", dpi, n_dp)):
        sq_all[at + idx] = sq[...]
        copies = [
            remote(sq, sq_all.at[at + idx], sq_send.at[at + k], sq_recv.at[at + k], {axis: lax.rem(idx + k, size)}) for k in range(1, size)
        ]
        for copy in copies:
            copy.start()
        if at == 0:
            gather_two(n_chunk - 1)
            gather_three(n_chunk - 2)
        for copy in copies:
            copy.wait()
        total = sq_all[at]
        for k in range(1, size):
            total = total + sq_all[at + k]
        sq[...] = total
        at += size
    gather_three(n_chunk - 1)
    total = jnp.sum(jnp.sum(sq[...], axis=0, keepdims=True), axis=1, keepdims=True) * (1.0 / (n_dp * n_dp))
    factor = (CLIP_NORM / jnp.maximum(jnp.sqrt(total), CLIP_NORM)) * (1.0 / n_dp)
    fac[...] = jnp.broadcast_to(factor, fac.shape)
    last = [pltpu.make_async_copy(fac, factor_out, out_sem.at[4])]
    for c in range(n_chunk):
        gather_four(c)
    for color in range(2):
        n = group_outs[2 * color].shape[0]
        for k, which in enumerate((core, 1 - core)):
            at = pl.ds(pl.multiple_of(which * n, 8), n)
            last.append(pltpu.make_async_copy(rings[color][1].at[at, :], group_outs[2 * color + k], out_sem.at[2 * color + k]))
    for copy in last:
        copy.start()

    for which, is_src, tok in ((0, src_h, lab), (1, src_x, ids)):

        @pl.when(is_src)
        def _(which=which, tok=tok):
            for k in range(1, n_pp):
                tok_copy(which, tok, k).wait_send()

    for c in range(n_chunk):
        for copy in rs_one(c) + rs_two(c):
            copy.wait_send()
    for copy in last:
        copy.wait()


def reduced_shards(master, acts, toks, sizes, chunks, bases, piece):
    n_tp, n_dp, n_pp = sizes
    block_rows, dim = master.shape
    tok_count = acts.shape[0]
    n_chunk = len(chunks)
    rows = n_chunk * n_dp * piece
    halves = [half_rows(sizes, chunks, piece, color) for color in (0, 0, 1, 1)]
    pieces = (tok_count // 2 // LANE + 1) // 2 * (LANE // PIECE_TOK)
    dma = pltpu.SemaphoreType.DMA
    f32, bf16 = jnp.float32, jnp.bfloat16
    outs = pl.pallas_call(
        functools.partial(front_kernel, (n_tp, n_dp, n_pp, chunks, bases, piece, block_rows)),
        out_shape=tuple(jax.ShapeDtypeStruct((n, dim), f32) for n in halves) + (jax.ShapeDtypeStruct((8, LANE), f32),),
        in_specs=[ANY, ANY, ANY],
        out_specs=(ANY,) * 5,
        scratch_shapes=[
            pltpu.VMEM((tok_count, dim), f32),
            pltpu.VMEM((tok_count, dim), f32),
            pltpu.VMEM((tok_count, dim), bf16),
            pltpu.VMEM((tok_count, dim), bf16),
            pltpu.VMEM((rows, dim), f32),
            pltpu.VMEM((rows, dim), bf16),
            pltpu.VMEM((rows, tok_count), f32),
            pltpu.VMEM((n_dp * piece, tok_count), bf16),
            pltpu.VMEM((1, tok_count), f32),
            pltpu.VMEM((n_pp, 1, tok_count), f32),
            pltpu.VMEM((n_tp, 1, tok_count), f32),
            pltpu.VMEM((n_chunk, 2, piece, dim // 2), f32),
            pltpu.VMEM((n_chunk, 2, piece, dim), f32),
            pltpu.VMEM((1, tok_count), jnp.int32),
            pltpu.VMEM((1, tok_count), jnp.int32),
            pltpu.VMEM((8, LANE), f32),
            pltpu.VMEM((n_pp + n_tp + n_dp, 8, LANE), f32),
            pltpu.VMEM((8, LANE), f32),
            dma((n_chunk,)),
            dma((2,)),
            dma((2, n_pp)),
            dma((2,)),
            dma((2, 4, pieces)),
            dma((2, 4)),
            dma((2, 2)),
            dma((2, 2)),
            dma((2, n_pp)),
            dma((2, n_pp)),
            dma((2, n_chunk, 2)),
            dma((2, n_chunk, 2)),
            dma((n_pp + n_tp + n_dp,)),
            dma((n_pp + n_tp + n_dp,)),
            dma((5,)),
            dma((n_chunk, 4)),
            dma((n_chunk, 4)),
            dma((n_chunk, 4)),
            dma((n_chunk, 4)),
            pltpu.SemaphoreType.REGULAR,
        ],
        compiler_params=pltpu.CompilerParams(collective_id=1, has_side_effects=True, vmem_limit_bytes=62 * 2**20),
        cost_estimate=pl.CostEstimate(flops=20 * 10**9, bytes_accessed=25 * 10**6, transcendentals=8 * 10**6),
        name="reduced_shards",
    )(master, acts, toks)
    return outs[:-1], outs[-1]


def adamw_kernel(n_prev, firsts, factor, *refs):
    n_seg = len(firsts)
    grads = refs[:n_seg]
    master, avg, avg_sq = refs[n_seg : n_seg + 3]
    new_master, new_avg, new_sq, new_bf = refs[n_seg + 3 + n_prev :]
    step = pl.program_id(0)
    g = grads[0][...]
    for first, ref in zip(firsts[1:], grads[1:], strict=True):
        g = jnp.where(step >= first, ref[...], g)
    g = g * factor[0:1, 0:1]
    m = BETA_ONE * avg[...] + (1.0 - BETA_ONE) * g
    v = BETA_TWO * avg_sq[...] + (1.0 - BETA_TWO) * g * g
    step_dir = (m * (1.0 / (1.0 - BETA_ONE**OPT_STEP))) / (jnp.sqrt(v * (1.0 / (1.0 - BETA_TWO**OPT_STEP))) + ADAM_EPS)
    w = master[...]
    w = w - LEARN_RATE * (step_dir + WEIGHT_DECAY * w)
    new_master[...] = w
    new_avg[...] = m
    new_sq[...] = v
    new_bf[...] = w.astype(jnp.bfloat16)


def update_rows(factor, segments, master, avg, avg_sq, prev, tile):
    block_rows, dim = master.shape
    counts = [-(-g.shape[0] // tile) for g, _ in segments]
    firsts = [sum(counts[:k]) for k in range(len(counts))]

    def local(k, i):
        rows = segments[k][0].shape[0]
        valid = jnp.minimum(rows, block_rows - segments[k][1]())
        return jnp.minimum(jnp.clip(i - firsts[k], 0, counts[k] - 1) * tile, valid - tile)

    def grad_index(k):
        return lambda i: (pl.multiple_of(local(k, i), 8), 0)

    def table_index(i):
        row = segments[0][1]() + local(0, i)
        for k in range(1, len(segments)):
            row = jnp.where(i >= firsts[k], segments[k][1]() + local(k, i), row)
        return pl.multiple_of(row, 8), 0

    shape = (pl.Element(tile), pl.Element(dim))
    table = pl.BlockSpec(shape, table_index)
    n_prev, n_seg = len(prev), len(segments)
    rows = sum(g.shape[0] for g, _ in segments)
    return pl.pallas_call(
        functools.partial(adamw_kernel, n_prev, firsts),
        grid=(sum(counts),),
        out_shape=(
            jax.ShapeDtypeStruct(master.shape, jnp.float32),
            jax.ShapeDtypeStruct(master.shape, jnp.float32),
            jax.ShapeDtypeStruct(master.shape, jnp.float32),
            jax.ShapeDtypeStruct(master.shape, jnp.bfloat16),
        ),
        in_specs=[pl.BlockSpec((8, LANE), lambda i: (0, 0))] + [pl.BlockSpec(shape, grad_index(k)) for k in range(n_seg)] + [table] * 3 + [ANY] * n_prev,
        out_specs=(table, table, table, table),
        input_output_aliases={4 + n_seg + i: i for i in range(n_prev)},
        compiler_params=pltpu.CompilerParams(vmem_limit_bytes=14 * 2**20),
        cost_estimate=pl.CostEstimate(flops=rows * dim * 2000, bytes_accessed=rows * dim * 30, transcendentals=rows * dim),
    )(factor, *[g for g, _ in segments], master, avg, avg_sq, *prev)


def half_rows(sizes, chunks, piece, color):
    _, n_dp, n_pp = sizes
    owners = n_pp if color == 0 else 2 * n_dp
    return owners // 2 * piece * sum(1 for k, _, _ in chunks if k == color)


def layout_of(block_rows, n_dp, n_pp):
    devices = n_dp * n_pp
    colors = (0, 1, 0, 1, 0)
    piece = -(-(-(-block_rows // (devices * len(colors)))) // 16) * 16
    chunks = tuple((k, colors[:i].count(k), colors.count(k)) for i, k in enumerate(colors))
    return piece, chunks, (0, devices * piece * colors.count(0))


def solution(mesh):
    n_tp, n_dp, n_pp = mesh.shape["tp"], mesh.shape["dp"], mesh.shape["pp"]
    n_x = n_pp // 2
    table_spec = P("tp", None)
    places = [(d, p) for d in range(n_dp) for p in range(n_pp)]

    def step_way(p):
        return 1 if p % 2 == 0 else -1

    col_ring = [(d * n_pp + p, (d + step_way(p)) % n_dp * n_pp + p) for d, p in places]
    row_ring = [(p, (p // 2 + step_way(p)) % n_x * 2 + p % 2) for p in range(n_pp)]
    swap = [(p, p ^ 1) for p in range(n_pp)]

    def along(color, val):
        return lax.ppermute(val, ("dp", "pp"), col_ring) if color == 0 else lax.ppermute(val, "pp", row_ring)

    def swapped(val):
        return lax.ppermute(val, "pp", swap)

    def device_step(master, exp_avg, exp_avg_sq, stage_ids, stage_acts):
        block_rows, dim = master.shape
        sizes = (n_tp, n_dp, n_pp)
        piece, chunks, bases = layout_of(block_rows, n_dp, n_pp)
        tok_count = stage_ids.shape[1] * stage_ids.shape[2]
        toks = stage_ids.reshape(1, tok_count)
        acts = stage_acts.reshape(tok_count, dim)
        groups, factor = reduced_shards(master, acts, toks, sizes, chunks, bases, piece)
        halves = [half_rows(sizes, chunks, piece, color) for color in range(2)]

        def segment(color, val, away, other):
            half = halves[color]

            def row():
                p = lax.axis_index("pp")
                core = lax.rem(p, 2)
                size = n_dp if color == 0 else n_x
                own = lax.axis_index("dp") if color == 0 else p // 2
                shift = away if away in (0, 2) else (2 * core - 1) * away
                group = lax.rem(own + shift + size, size)
                return bases[color] + (group * 2 + (1 - core if other else core)) * half

            return val, row

        first, second = groups[0::2], groups[1::2]
        ring_first = [along(k, first[k]) for k in range(2)]
        ring_second = [along(k, second[k]) for k in range(2)]
        swap_first = [swapped(ring_first[k]) for k in range(2)]
        far = [along(k, ring_first[k]) for k in range(2)]
        swap_second = [swapped(ring_second[k]) for k in range(2)]
        swap_far = [swapped(far[k]) for k in range(2)]
        spare = block_rows - bases[1] - (2 * n_x - 1) * halves[1]
        tile = min(160, spare // 8 * 8)
        plan = (
            [segment(k, v[k], 0, o) for o, v in ((False, first), (True, second)) for k in range(2)],
            [segment(k, ring_first[k], 1, False) for k in range(2)],
            [segment(k, swap_first[k], -1, True) for k in range(2)],
            [segment(k, ring_second[k], 1, True) for k in range(2)],
            [segment(k, swap_second[k], -1, False) for k in range(2)],
            [segment(k, far[k], 2, False) for k in range(2)],
            [segment(k, swap_far[k], 2, True) for k in range(2)],
        )
        outs = ()
        for segments in plan:
            outs = tuple(update_rows(factor, segments, master, exp_avg, exp_avg_sq, outs, tile))
        return outs

    specs = (table_spec, table_spec, table_spec, P("pp", "dp", None), P("pp", "dp", None, None))

    return jax.shard_map(device_step, mesh=mesh, in_specs=specs, out_specs=(table_spec,) * 4, check_vma=False)
```

```python
import functools

import jax
import jax.numpy as jnp
from jax import lax
from jax.experimental import pallas as pl
from jax.experimental.pallas import tpu as pltpu
from jax.sharding import PartitionSpec as P


LEARN_RATE = 0.003
BETA_ONE = 0.9
BETA_TWO = 0.95
ADAM_EPS = 1e-8
WEIGHT_DECAY = 0.1
CLIP_NORM = 1.0
OPT_STEP = 10


MESH = pl.DeviceIdType.MESH
ANY = pl.BlockSpec(memory_space=pl.ANY)
VMEM = pl.BlockSpec(memory_space=pltpu.VMEM)
NEG_BIG = float("-inf")


def in_block(local, block_rows):
    return jnp.where(local < block_rows, local, -(2**30))


def remote(src, dst, send_sem, recv_sem, device):
    return pltpu.make_async_remote_copy(
        src_ref=src, dst_ref=dst, send_sem=send_sem, recv_sem=recv_sem, device_id=device, device_id_type=MESH
    )


LANE = 128
PIECE_TOK = 64


def front_kernel(
    cfg, master, acts, toks, *refs
):
    n_tp, n_dp, n_pp, chunks, bases, piece, block_rows = cfg
    group_outs, factor_out = refs[:4], refs[4]
    (h_f, x_f, h_bf, x_bf, part, e_bf, logit, dlog, lse, lse_a, lse_b, rs_a, rs_b, lab, ids, sq, sq_all, fac) = refs[5:23]
    (e_sem, load_sem, tok_send, tok_recv, st_recv, d2d_send, x_send, z_send, lse_send, lse_recv, rs_send, rs_recv, sq_send, sq_recv, out_sem) = refs[23:38]
    (f_send, f_recv, p_send, p_recv, ready) = refs[38:]
    me = lax.axis_index("pp")
    tpi = lax.axis_index("tp")
    dpi = lax.axis_index("dp")
    n_x = n_pp // 2
    x, core = me // 2, lax.rem(me, 2)
    n_chunk = len(chunks)
    rows_chunk = n_dp * piece
    tok_count, dim = h_f.shape
    half_tok = tok_count // 2
    tiles_a = (half_tok // LANE + 1) // 2
    tiles_b = half_tok // LANE - tiles_a
    per_tile = LANE // PIECE_TOK
    counts = (tiles_a * per_tile, tiles_b * per_tile) * 2
    tok_a = tiles_a * LANE

    def row_at(c, d, x_at, core_at):
        color, s, count = chunks[c]
        owner = d * n_pp + x_at * 2 + core_at if color == 0 else x_at * (2 * n_dp) + d * 2 + core_at
        return bases[color] + (owner * count + s) * piece

    def first_row(c, d):
        return row_at(c, d, x, core)

    def whole(c, d):
        return row_at(c, d, n_x - 1, 1) + piece <= block_rows

    tail = block_rows % piece

    def row_copy(c, d, n):
        slot = c * rows_chunk + d * piece
        start = pl.multiple_of(first_row(c, d), 8)
        return pltpu.make_async_copy(master.at[pl.ds(start, n), :], part.at[pl.ds(slot, n), :], e_sem.at[c])

    def on_rows(act):
        for c in range(n_chunk):
            for d in range(n_dp):
                if whole(c, d):
                    act(row_copy(c, d, piece))
                else:

                    @pl.when(first_row(c, d) + piece <= block_rows)
                    def _(c=c, d=d):
                        act(row_copy(c, d, piece))

                    if tail:

                        @pl.when(first_row(c, d) + tail == block_rows)
                        def _(c=c, d=d):
                            act(row_copy(c, d, tail))

    src_h = me == n_pp - 1
    src_x = me == 0

    def source_loads(buf, tok):
        return (pltpu.make_async_copy(acts, buf, load_sem.at[0]), pltpu.make_async_copy(toks, tok, load_sem.at[1]))

    for is_src, buf, tok in ((src_h, h_bf, lab), (src_x, x_bf, ids)):

        @pl.when(is_src)
        def _(buf=buf, tok=tok):
            for c in source_loads(buf, tok):
                c.start()

    on_rows(lambda c: c.start())
    barrier = pltpu.get_barrier_semaphore()
    for axis, idx, size in (("pp", me, n_pp), ("tp", tpi, n_tp), ("dp", dpi, n_dp)):
        for k in range(1, size):
            pl.semaphore_signal(barrier, inc=1, device_id={axis: lax.rem(idx + k, size)}, device_id_type=MESH)

    def widen(buf, wide):
        def one(t, _):
            at = pl.ds(pl.multiple_of(t * LANE, LANE), LANE)
            wide[at, :] = buf[at, :].astype(jnp.float32)
            return 0

        return one

    @pl.when(src_h)
    def _():
        for c in source_loads(h_bf, lab):
            c.wait()
        for t in (0, tok_a, half_tok, half_tok + tok_a):
            widen(h_bf, h_f)(t // LANE, 0)

    pl.semaphore_wait(barrier, n_pp + n_tp + n_dp - 3)

    def tok_copy(which, ref, k):
        return remote(ref, ref, tok_send.at[which, k], tok_recv.at[which], {"pp": lax.rem(me + k, n_pp)})

    half = lax.rem(tpi, 2)
    partner = {"pp": x * 2 + 1 - core}
    right = {"pp": lax.rem(x + 1, n_x) * 2 + core}
    left = {"pp": lax.rem(x + n_x - 1, n_x) * 2 + core}
    z_up = {"tp": lax.rem(tpi + 1, n_tp)}
    z_down = {"tp": lax.rem(tpi + n_tp - 1, n_tp)}
    hop = 2 * per_tile // 2
    lag = (hop * (n_x - 2) + hop) // per_tile + 1

    def stream(s, buf, lead=0):
        handler = core == 1 - s
        u = lax.rem(x - (n_x - 1, 0)[s] + n_x, n_x)
        base = [half * half_tok, half * half_tok + tok_a, (1 - half) * half_tok, (1 - half) * half_tok + tok_a]
        ahead = jnp.maximum(u - 1, 0) * hop
        behind = jnp.where(u == 0, 0, (n_x - 1 - u) * hop)
        second = jnp.where(u == 0, 0, hop)
        early = jnp.where(handler & (u == 0), lead * per_tile, 0)
        offs = (ahead - early, behind - early, ahead + second - early, behind + second - early)

        def rows(kind, p, n):
            return buf.at[pl.ds(pl.multiple_of(base[kind] + p * PIECE_TOK, PIECE_TOK), n), :]

        def copy(kind, p, to, sem, device, n=PIECE_TOK):
            at = rows(kind, p, n)
            return remote(at, at, sem, st_recv.at[s, to, p], device)

        def outs(kind):
            found = [(handler, kind, d2d_send.at[s, kind], partner)]
            if kind == 0:
                found.append((handler & (u <= n_x - 2), 0, x_send.at[s, 0], right))
                found.append((handler & (u > 0), 2, z_send.at[s, 0], z_up))
            if kind == 1:
                found.append((handler & ((u == 0) | (u >= 2)), 1, x_send.at[s, 1], left))
                found.append((handler & (u > 0), 3, z_send.at[s, 1], z_down))
            return found

        def slot(t):
            for kind in range(4):
                p = t - offs[kind]

                @pl.when((p >= 0) & (p < counts[kind]))
                def _(kind=kind, p=p):
                    @pl.when(jnp.logical_not(handler & (u == 0)))
                    def _():
                        copy(kind, p, kind, d2d_send.at[s, kind], partner).wait_recv()

                    for cond, to, sem, device in reversed(outs(kind)):

                        @pl.when(cond)
                        def _(to=to, sem=sem, device=device):
                            copy(kind, p, to, sem, device).start()

        def drain():
            for kind in range(4):
                for cond, to, sem, device in outs(kind):

                    @pl.when(cond)
                    def _(kind=kind, to=to, sem=sem, device=device):
                        copy(kind, 0, to, sem, device, counts[kind] * PIECE_TOK).wait_send()

        return slot, drain

    h_slot, h_drain = stream(0, h_f)
    n_it = lag + tiles_b
    x_first = n_it - 1
    x_slot, x_drain = stream(1, x_f, x_first - tiles_a)

    def x_it(it):
        for k in range(per_tile):
            x_slot(it * per_tile + k)

    def prepare_rows():
        on_rows(lambda c: c.wait())
        for c in range(n_chunk):
            for d in range(n_dp):
                at = pl.ds(c * rows_chunk + d * piece, piece)
                rows = part[at, :]
                if not whole(c, d):
                    inside = lax.broadcasted_iota(jnp.int32, (piece, dim), 0) + first_row(c, d) < block_rows
                    rows = jnp.where(inside, rows, 0.0)
                e_bf[at, :] = rows.astype(jnp.bfloat16)

    wide_tile = 2 * LANE

    def logit_pair(t_one, t_two):
        ats = [pl.ds(pl.multiple_of(t, LANE), LANE) for t in (t_one, t_two)]
        h_tile = jnp.concatenate([h_f[at, :].astype(jnp.bfloat16) for at in ats], axis=0)
        for i, at in enumerate(ats):
            h_bf[at, :] = h_tile[i * LANE : (i + 1) * LANE]
        top = jnp.full((8, wide_tile), NEG_BIG, jnp.float32)
        iota_p = lax.broadcasted_iota(jnp.int32, (piece, wide_tile), 0)
        for c in range(n_chunk):
            rows = pl.ds(c * rows_chunk, rows_chunk)
            val = lax.dot_general(e_bf[rows, :], h_tile, (((1,), (1,)), ((), ())), preferred_element_type=jnp.float32)
            for d in range(n_dp):
                sub = val[d * piece : (d + 1) * piece]
                if not whole(c, d):
                    sub = jnp.where(iota_p + first_row(c, d) < block_rows, sub, NEG_BIG)
                for i, at in enumerate(ats):
                    logit[pl.ds(c * rows_chunk + d * piece, piece), at] = sub[:, i * LANE : (i + 1) * LANE]
                top = jnp.maximum(top, jnp.max(sub.reshape(piece // 8, 8, wide_tile), axis=0))
        top = jnp.max(top, axis=0, keepdims=True)
        for i, at in enumerate(ats):
            peak = top[:, i * LANE : (i + 1) * LANE]
            total = jnp.zeros((8, LANE), jnp.float32)
            for c in range(n_chunk):
                val = jnp.exp(logit[pl.ds(c * rows_chunk, rows_chunk), at] - peak)
                total = total + jnp.sum(val.reshape(rows_chunk // 8, 8, LANE), axis=0)
            lse[:, at] = peak + jnp.log(jnp.sum(total, axis=0, keepdims=True))

    def h_only(it, _):
        for k in range(per_tile):
            h_slot(it * per_tile + k)
        return 0

    def h_and_logits(it, _):
        j = it - lag
        for k in range(per_tile):
            h_slot(it * per_tile + k)
            x_slot((it - x_first) * per_tile + k)
            if k < 2:
                logit_pair(k * half_tok + j * LANE, k * half_tok + tok_a + j * LANE)
        return 0

    @pl.when(src_h)
    def _():
        h_only(0, 0)
        for t, n in ((0, tiles_a), (tiles_a, tiles_b), (tiles_a + tiles_b, tiles_a), (2 * tiles_a + tiles_b, tiles_b)):
            lax.fori_loop(t + 1, t + n, widen(h_bf, h_f), 0)

    prepare_rows()

    @pl.when(src_x)
    def _():
        for c in source_loads(x_bf, ids):
            c.wait()
        lax.fori_loop(0, tok_count // LANE, widen(x_bf, x_f), 0)

    for which, is_src, tok in ((0, src_h, lab), (1, src_x, ids)):

        @pl.when(is_src)
        def _(which=which, tok=tok):
            for k in range(1, n_pp):
                tok_copy(which, tok, k).start()

    @pl.when(jnp.logical_not(src_h))
    def _():
        h_only(0, 0)

    lax.fori_loop(1, lag, h_only, 0)
    lax.fori_loop(lag, n_it, h_and_logits, 0)
    logit_pair((tiles_a - 1) * LANE, half_tok + (tiles_a - 1) * LANE)
    x_done = n_it - x_first

    def lse_copy(axis, idx, size, gathered, stage, k):
        return remote(lse, gathered.at[k], lse_send.at[stage, k], lse_recv.at[stage, k], {axis: lax.rem(idx + k, size)})

    def lse_finish(copies, gathered, size):
        own = lse[...]
        for copy in copies:
            copy.wait()
        top = own
        for k in range(1, size):
            top = jnp.maximum(top, gathered[k])
        total = jnp.exp(own - top)
        for k in range(1, size):
            total = total + jnp.exp(gathered[k] - top)
        lse[...] = top + jnp.log(total)

    for stage, (axis, idx, size, gathered) in enumerate((("pp", me, n_pp, lse_a), ("tp", tpi, n_tp, lse_b))):
        copies = [lse_copy(axis, idx, size, gathered, stage, k) for k in range(1, size)]
        for copy in copies:
            copy.start()
        x_it(x_done + stage)
        lse_finish(copies, gathered, size)
    x_done += 2

    @pl.when(jnp.logical_not(src_h))
    def _():
        tok_copy(0, lab, 1).wait_recv()

    inv_tok = 1.0 / tok_count
    n_wide = tok_count // wide_tile
    iota_w = lax.broadcasted_iota(jnp.int32, (piece, wide_tile), 0)
    vocab_base = tpi * block_rows

    def dlog_chunk(c):
        def tile(t, _):
            at = pl.ds(pl.multiple_of(t * wide_tile, wide_tile), wide_tile)
            norm = lse[:, at]
            labels = in_block(lab[:, at] - vocab_base, block_rows)
            for d in range(n_dp):
                prob = jnp.exp(logit[pl.ds(c * rows_chunk + d * piece, piece), at] - norm)
                hit = iota_w == labels - first_row(c, d)
                dlog[pl.ds(d * piece, piece), at] = (jnp.where(hit, prob - 1.0, prob) * inv_tok).astype(jnp.bfloat16)
            return 0

        lax.fori_loop(0, n_wide, tile, 0)

    def times(tokens, add):
        def go(c):
            rows = pl.ds(c * rows_chunk, rows_chunk)
            val = jnp.dot(dlog[...], tokens[...], preferred_element_type=jnp.float32)
            part[rows, :] = part[rows, :] + val if add else val

        return go

    head = times(h_bf, False)
    look = times(x_bf, True)
    x_its = tiles_a + lag - 1
    for c in range(n_chunk):
        if x_done < x_its:
            x_it(x_done)
            x_done += 1
        dlog_chunk(c)
        head(c)
    while x_done < x_its:
        x_it(x_done)
        x_done += 1

    @pl.when(jnp.logical_not(src_x))
    def _():
        tok_copy(1, ids, 1).wait_recv()

    def narrow(t, _):
        at = pl.ds(pl.multiple_of(t * LANE, LANE), LANE)
        x_bf[at, :] = x_f[at, :].astype(jnp.bfloat16)
        return 0

    lax.fori_loop(0, tok_count // LANE, narrow, 0)

    def one_hot_chunk(c):
        def tile(t, _):
            at = pl.ds(pl.multiple_of(t * wide_tile, wide_tile), wide_tile)
            rows = in_block(ids[:, at] - vocab_base, block_rows)
            for d in range(n_dp):
                hit = iota_w == rows - first_row(c, d)
                dlog[pl.ds(d * piece, piece), at] = jnp.where(hit, 1.0, 0.0).astype(jnp.bfloat16)
            return 0

        lax.fori_loop(0, n_wide, tile, 0)

    up, down, far = lax.rem(dpi + 1, 4), lax.rem(dpi + 3, 4), lax.rem(dpi + 2, 4)
    hd = dim // 2

    def rows_of(c, d):
        return pl.ds(pl.multiple_of(c * rows_chunk + d * piece, 16), piece)

    def rs_one(c):
        return (
            remote(part.at[rows_of(c, far), pl.ds(0, hd)], rs_a.at[c, 0], rs_send.at[0, c, 0], rs_recv.at[0, c, 0], {"dp": up}),
            remote(part.at[rows_of(c, far), pl.ds(hd, hd)], rs_a.at[c, 1], rs_send.at[0, c, 1], rs_recv.at[0, c, 1], {"dp": down}),
        )

    def rs_two(c):
        return (
            remote(part.at[rows_of(c, up), :], rs_b.at[c, 0], rs_send.at[1, c, 0], rs_recv.at[1, c, 0], {"dp": up}),
            remote(part.at[rows_of(c, down), :], rs_b.at[c, 1], rs_send.at[1, c, 1], rs_recv.at[1, c, 1], {"dp": down}),
        )

    def merge(c):
        for copy in rs_one(c):
            copy.wait_recv()
        part[rows_of(c, up), pl.ds(0, hd)] += rs_a[c, 0]
        part[rows_of(c, down), pl.ds(hd, hd)] += rs_a[c, 1]
        for copy in rs_two(c):
            copy.start()

    rings = (
        ("pp", h_f, x, n_x, lambda q: q * 2 + core),
        ("dp", x_f, dpi, n_dp, lambda q: q),
    )

    def block(c, q, core_at, first=0, n=piece):
        color, s, count = chunks[c]
        return rings[color][1].at[pl.ds(pl.multiple_of(((q * 2 + core_at) * count + s) * piece + first, 8), n), :]

    def ring_copy(c, q, way, sem, first=0, n=piece):
        axis, _, idx, size, device = rings[chunks[c][0]]
        to = device(lax.rem(idx + (1 if way == 0 else size - 1), size))
        at = block(c, q, core, first, n)
        return remote(at, at, f_send.at[c, sem], f_recv.at[c, sem], {axis: to})

    def share(c, k):
        _, _, idx, size, _ = rings[chunks[c][0]]
        at = block(c, lax.rem(idx + k, size), core)
        return remote(at, at, p_send.at[c, k], p_recv.at[c, k], partner)

    cut = piece // 2

    def forwards(c):
        _, _, idx, size, _ = rings[chunks[c][0]]
        return (
            ring_copy(c, lax.rem(idx + size - 1, size), 0, 2, 0, cut),
            ring_copy(c, lax.rem(idx + 1, size), 1, 3, cut, piece - cut),
        )

    def owns(c):
        idx = rings[chunks[c][0]][2]
        return ring_copy(c, idx, 0, 0), ring_copy(c, idx, 1, 1)

    def gather_one(c):
        if c == 0:
            pl.semaphore_wait(ready, 5)
        for copy in owns(c):
            copy.start()
        share(c, 0).start()

    def gather_two(c):
        for own, forward, k in zip(owns(c), forwards(c), (3, 1), strict=True):
            own.wait_recv()
            forward.start()
            share(c, k).start()

    def gather_three(c):
        for copy in forwards(c):
            copy.wait_recv()
        share(c, 2).start()

    def gather_four(c):
        for k in range(4):
            share(c, k).wait()
        for copy in owns(c) + forwards(c):
            copy.wait_send()

    def final(c):
        for copy in rs_two(c):
            copy.wait_recv()
        val = part[rows_of(c, dpi), :] + rs_b[c, 0] + rs_b[c, 1]
        color, s, count = chunks[c]
        own = (rings[color][2] * 2 + core) * count + s
        rings[color][1][pl.ds(pl.multiple_of(own * piece, 8), piece), :] = val
        squares = val * val
        squares = jnp.sum(squares.reshape(piece // 8, 8, dim), axis=0)
        tile = squares[:, :LANE]
        for i in range(1, dim // LANE):
            tile = tile + squares[:, i * LANE : (i + 1) * LANE]
        sq[...] = tile if c == 0 else sq[...] + tile

    h_drain()
    x_drain()
    for device in (right, left, partner, {"dp": up}, {"dp": down}):
        pl.semaphore_signal(ready, inc=1, device_id=device, device_id_type=MESH)

    for c in range(n_chunk + 4):
        if c < n_chunk:
            one_hot_chunk(c)
            look(c)
            for copy in rs_one(c):
                copy.start()
        if 0 <= c - 2 < n_chunk:
            merge(c - 2)
        if 0 <= c - 4 < n_chunk:
            final(c - 4)
            gather_one(c - 4)
        if 0 <= c - 5 < n_chunk:
            gather_two(c - 5)
        if 0 <= c - 6 < n_chunk:
            gather_three(c - 6)

    at = 0
    for axis, idx, size in (("pp", me, n_pp), ("tp", tpi, n_tp), ("dp", dpi, n_dp)):
        sq_all[at + idx] = sq[...]
        copies = [
            remote(sq, sq_all.at[at + idx], sq_send.at[at + k], sq_recv.at[at + k], {axis: lax.rem(idx + k, size)}) for k in range(1, size)
        ]
        for copy in copies:
            copy.start()
        if at == 0:
            gather_two(n_chunk - 1)
            gather_three(n_chunk - 2)
        for copy in copies:
            copy.wait()
        total = sq_all[at]
        for k in range(1, size):
            total = total + sq_all[at + k]
        sq[...] = total
        at += size
    gather_three(n_chunk - 1)
    total = jnp.sum(jnp.sum(sq[...], axis=0, keepdims=True), axis=1, keepdims=True) * (1.0 / (n_dp * n_dp))
    factor = (CLIP_NORM / jnp.maximum(jnp.sqrt(total), CLIP_NORM)) * (1.0 / n_dp)
    fac[...] = jnp.broadcast_to(factor, fac.shape)
    last = [pltpu.make_async_copy(fac, factor_out, out_sem.at[4])]
    last[0].start()
    for color in range(2):
        for c in range(n_chunk):
            if chunks[c][0] == color:
                gather_four(c)
        n = group_outs[2 * color].shape[0]
        for k, which in enumerate((core, 1 - core)):
            at = pl.ds(pl.multiple_of(which * n, 8), n)
            last.append(pltpu.make_async_copy(rings[color][1].at[at, :], group_outs[2 * color + k], out_sem.at[2 * color + k]))
            last[-1].start()

    for which, is_src, tok in ((0, src_h, lab), (1, src_x, ids)):

        @pl.when(is_src)
        def _(which=which, tok=tok):
            for k in range(1, n_pp):
                tok_copy(which, tok, k).wait_send()

    for c in range(n_chunk):
        for copy in rs_one(c) + rs_two(c):
            copy.wait_send()
    for copy in last:
        copy.wait()


def reduced_shards(master, acts, toks, sizes, chunks, bases, piece):
    n_tp, n_dp, n_pp = sizes
    block_rows, dim = master.shape
    tok_count = acts.shape[0]
    n_chunk = len(chunks)
    rows = n_chunk * n_dp * piece
    halves = [half_rows(sizes, chunks, piece, color) for color in (0, 0, 1, 1)]
    pieces = (tok_count // 2 // LANE + 1) // 2 * (LANE // PIECE_TOK)
    dma = pltpu.SemaphoreType.DMA
    f32, bf16 = jnp.float32, jnp.bfloat16
    outs = pl.pallas_call(
        functools.partial(front_kernel, (n_tp, n_dp, n_pp, chunks, bases, piece, block_rows)),
        out_shape=tuple(jax.ShapeDtypeStruct((n, dim), f32) for n in halves) + (jax.ShapeDtypeStruct((8, LANE), f32),),
        in_specs=[ANY, ANY, ANY],
        out_specs=(ANY,) * 5,
        scratch_shapes=[
            pltpu.VMEM((tok_count, dim), f32),
            pltpu.VMEM((tok_count, dim), f32),
            pltpu.VMEM((tok_count, dim), bf16),
            pltpu.VMEM((tok_count, dim), bf16),
            pltpu.VMEM((rows, dim), f32),
            pltpu.VMEM((rows, dim), bf16),
            pltpu.VMEM((rows, tok_count), f32),
            pltpu.VMEM((n_dp * piece, tok_count), bf16),
            pltpu.VMEM((1, tok_count), f32),
            pltpu.VMEM((n_pp, 1, tok_count), f32),
            pltpu.VMEM((n_tp, 1, tok_count), f32),
            pltpu.VMEM((n_chunk, 2, piece, dim // 2), f32),
            pltpu.VMEM((n_chunk, 2, piece, dim), f32),
            pltpu.VMEM((1, tok_count), jnp.int32),
            pltpu.VMEM((1, tok_count), jnp.int32),
            pltpu.VMEM((8, LANE), f32),
            pltpu.VMEM((n_pp + n_tp + n_dp, 8, LANE), f32),
            pltpu.VMEM((8, LANE), f32),
            dma((n_chunk,)),
            dma((2,)),
            dma((2, n_pp)),
            dma((2,)),
            dma((2, 4, pieces)),
            dma((2, 4)),
            dma((2, 2)),
            dma((2, 2)),
            dma((2, n_pp)),
            dma((2, n_pp)),
            dma((2, n_chunk, 2)),
            dma((2, n_chunk, 2)),
            dma((n_pp + n_tp + n_dp,)),
            dma((n_pp + n_tp + n_dp,)),
            dma((5,)),
            dma((n_chunk, 4)),
            dma((n_chunk, 4)),
            dma((n_chunk, 4)),
            dma((n_chunk, 4)),
            pltpu.SemaphoreType.REGULAR,
        ],
        compiler_params=pltpu.CompilerParams(collective_id=1, has_side_effects=True, vmem_limit_bytes=62 * 2**20),
        cost_estimate=pl.CostEstimate(flops=20 * 10**9, bytes_accessed=25 * 10**6, transcendentals=8 * 10**6),
        name="reduced_shards",
    )(master, acts, toks)
    return outs[:-1], outs[-1]


def in_hbm(val):
    return pltpu.with_memory_space_constraint(val, pltpu.HBM)


SLAB = 16


def adamw_kernel(n_prev, firsts, factor, *refs):
    n_seg = len(firsts)
    grads = refs[:n_seg]
    master, avg, avg_sq = refs[n_seg : n_seg + 3]
    new_master, new_avg, new_sq, new_bf = refs[n_seg + 3 + n_prev :]
    step = pl.program_id(0)
    scale = factor[0:1, 0:1]
    rows, _ = new_master.shape
    slab = min(SLAB, rows)

    def some_rows(i, _):
        at = pl.ds(pl.multiple_of(i * slab, slab), slab)
        g = grads[0][at, :]
        for first, ref in zip(firsts[1:], grads[1:], strict=True):
            g = jnp.where(step >= first, ref[at, :], g)
        g = g * scale
        m = BETA_ONE * avg[at, :] + (1.0 - BETA_ONE) * g
        v = BETA_TWO * avg_sq[at, :] + (1.0 - BETA_TWO) * g * g
        new_avg[at, :] = m
        new_sq[at, :] = v
        step_dir = (m * (1.0 / (1.0 - BETA_ONE**OPT_STEP))) / (jnp.sqrt(v * (1.0 / (1.0 - BETA_TWO**OPT_STEP))) + ADAM_EPS)
        w = master[at, :]
        w = w - LEARN_RATE * (step_dir + WEIGHT_DECAY * w)
        new_master[at, :] = w
        new_bf[at, :] = w.astype(jnp.bfloat16)
        return 0

    lax.fori_loop(0, rows // slab, some_rows, 0)


def update_rows(factor, segments, master, avg, avg_sq, prev, tile):
    block_rows, dim = master.shape
    counts = [-(-g.shape[0] // tile) for g, _ in segments]
    firsts = [sum(counts[:k]) for k in range(len(counts))]

    def local(k, i):
        rows = segments[k][0].shape[0]
        valid = jnp.minimum(rows, block_rows - segments[k][1]())
        return jnp.minimum(jnp.clip(i - firsts[k], 0, counts[k] - 1) * tile, valid - tile)

    def grad_index(k):
        return lambda i: (pl.multiple_of(local(k, i), 8), 0)

    def table_index(i):
        row = segments[0][1]() + local(0, i)
        for k in range(1, len(segments)):
            row = jnp.where(i >= firsts[k], segments[k][1]() + local(k, i), row)
        return pl.multiple_of(row, 8), 0

    shape = (pl.Element(tile), pl.Element(dim))
    table = pl.BlockSpec(shape, table_index)
    n_prev, n_seg = len(prev), len(segments)
    rows = sum(g.shape[0] for g, _ in segments)
    return pl.pallas_call(
        functools.partial(adamw_kernel, n_prev, firsts),
        grid=(sum(counts),),
        out_shape=(
            jax.ShapeDtypeStruct(master.shape, jnp.float32),
            jax.ShapeDtypeStruct(master.shape, jnp.float32),
            jax.ShapeDtypeStruct(master.shape, jnp.float32),
            jax.ShapeDtypeStruct(master.shape, jnp.bfloat16),
        ),
        in_specs=[pl.BlockSpec((8, LANE), lambda i: (0, 0))] + [pl.BlockSpec(shape, grad_index(k)) for k in range(n_seg)] + [table] * 3 + [ANY] * n_prev,
        out_specs=(table, table, table, table),
        input_output_aliases={4 + n_seg + i: i for i in range(n_prev)},
        compiler_params=pltpu.CompilerParams(vmem_limit_bytes=14 * 2**20),
        cost_estimate=pl.CostEstimate(flops=rows * dim * 2000, bytes_accessed=rows * dim * 30, transcendentals=rows * dim),
    )(in_hbm(factor), *[g for g, _ in segments], *[in_hbm(v) for v in (master, avg, avg_sq)], *prev)


def half_rows(sizes, chunks, piece, color):
    _, n_dp, n_pp = sizes
    owners = n_pp if color == 0 else 2 * n_dp
    return owners // 2 * piece * sum(1 for k, _, _ in chunks if k == color)


def layout_of(block_rows, n_dp, n_pp):
    devices = n_dp * n_pp
    colors = (0, 0, 1, 0, 1)
    piece = -(-(-(-block_rows // (devices * len(colors)))) // 16) * 16
    chunks = tuple((k, colors[:i].count(k), colors.count(k)) for i, k in enumerate(colors))
    return piece, chunks, (0, devices * piece * colors.count(0))


def solution(mesh):
    n_tp, n_dp, n_pp = mesh.shape["tp"], mesh.shape["dp"], mesh.shape["pp"]
    n_x = n_pp // 2
    table_spec = P("tp", None)
    places = [(d, p) for d in range(n_dp) for p in range(n_pp)]

    def step_way(p):
        return 1 if p % 2 == 0 else -1

    col_ring = [(d * n_pp + p, (d + step_way(p)) % n_dp * n_pp + p) for d, p in places]
    row_ring = [(p, (p // 2 + step_way(p)) % n_x * 2 + p % 2) for p in range(n_pp)]
    swap = [(p, p ^ 1) for p in range(n_pp)]

    def along(color, val):
        return lax.ppermute(val, ("dp", "pp"), col_ring) if color == 0 else lax.ppermute(val, "pp", row_ring)

    def swapped(val):
        return lax.ppermute(val, "pp", swap)

    def device_step(master, exp_avg, exp_avg_sq, stage_ids, stage_acts):
        block_rows, dim = master.shape
        sizes = (n_tp, n_dp, n_pp)
        piece, chunks, bases = layout_of(block_rows, n_dp, n_pp)
        tok_count = stage_ids.shape[1] * stage_ids.shape[2]
        toks = stage_ids.reshape(1, tok_count)
        acts = stage_acts.reshape(tok_count, dim)
        groups, factor = reduced_shards(master, acts, toks, sizes, chunks, bases, piece)
        halves = [half_rows(sizes, chunks, piece, color) for color in range(2)]

        def segment(color, val, away, other):
            half = halves[color]

            def row():
                p = lax.axis_index("pp")
                core = lax.rem(p, 2)
                size = n_dp if color == 0 else n_x
                own = lax.axis_index("dp") if color == 0 else p // 2
                shift = away if away in (0, 2) else (2 * core - 1) * away
                group = lax.rem(own + shift + size, size)
                return bases[color] + (group * 2 + (1 - core if other else core)) * half

            return val, row

        first, second = groups[0::2], groups[1::2]
        ring_first = [along(k, first[k]) for k in range(2)]
        ring_second = [along(k, second[k]) for k in range(2)]
        swap_first = [swapped(ring_first[k]) for k in range(2)]
        far = [along(k, ring_first[k]) for k in range(2)]
        swap_second = [swapped(ring_second[k]) for k in range(2)]
        swap_far = [swapped(far[k]) for k in range(2)]
        spare = block_rows - bases[1] - (2 * n_x - 1) * halves[1]
        tile = min(160, spare // 8 * 8)
        plan = (
            [segment(k, in_hbm(v[k]), 0, o) for o, v in ((False, first), (True, second)) for k in range(2)],
            [segment(k, ring_first[k], 1, False) for k in range(2)],
            [segment(k, swap_first[k], -1, True) for k in range(2)],
            [segment(k, ring_second[k], 1, True) for k in range(2)],
            [segment(k, swap_second[k], -1, False) for k in range(2)],
            [segment(k, far[k], 2, False) for k in range(2)],
            [segment(k, swap_far[k], 2, True) for k in range(2)],
        )
        outs = ()
        for segments in plan:
            outs = tuple(update_rows(factor, segments, master, exp_avg, exp_avg_sq, outs, tile))
        return outs

    specs = (table_spec, table_spec, table_spec, P("pp", "dp", None), P("pp", "dp", None, None))

    return jax.shard_map(device_step, mesh=mesh, in_specs=specs, out_specs=(table_spec,) * 4, check_vma=False)
```
